32 devices in a mesh: dom: 16 (over z, y, x), sub: 2 (over core).
Axes of the slice: x: 2, y: 2, z: 4, core: 2. Of those that a mesh axis runs over, the one named last changes fastest.
Arguments:
- old_states: bfloat16 [512, 320], P(('dom', 'sub')), may hold values from -6 to 6
- send_elem: int32 [32, 9, 8], P(('dom', 'sub')), may hold values from -1 to 15, as said below
- recv_slot: int32 [512, 4], P(('dom', 'sub')), may hold values from -1 to 71, as said below
- intersection_count: int32 [512], P(('dom', 'sub')), may hold values from 1 to 4
- intersection_weight: float32 [512, 4], P(('dom', 'sub')), may hold values from 0.1 to 1
- interior_inverse: bfloat16 [512, 320, 320], P(('dom', 'sub')), may hold values from -0.3125 to 0.3125
- inner_coupling: bfloat16 [512, 320, 400], P(('dom', 'sub')), may hold values from -6 to 6
- face_coupling: bfloat16 [512, 400, 320], P(('dom', 'sub')), may hold values from -0.3125 to 0.3125
- face_mass: float32 [80, 80], replicated, may hold values from -6 to 6
- face_scale: float32 [512, 5], P(('dom', 'sub')), may hold values from 0.5 to 2
- face_shift: int32 [512, 5], P(('dom', 'sub')), may hold values from -4 to 4, as said below
- owner_row: int32 [32, 9, 9], P(('dom', 'sub')), may hold values from -1 to 39, as said below
Outputs:
- face_schur: float32 [1280, 6400], P(('dom', 'sub'))
- face_rhs: float32 [1280, 80], P(('dom', 'sub'))
The draws below stay inside these ranges and needn't reach their ends.
Inputs may be any that keep to these rules, and one draw needn't show every extreme that they name: `send_elem`: -1 marks an empty slot. For every live entry of recv_slot the named slot holds an element of the source; no slot is named twice; some old owner fills all 8 slots toward one new owner. `recv_slot`: entry k of new element n is -1 exactly when k >= intersection_count[n], else the index of a filled slot. `face_shift`: on one device at most 9 items share a shift value, and some value has exactly 9. `owner_row`: -1 exactly where no item arrives; every owned row is named by exactly two arriving items.
All inputs are finite; a program needn't handle non-finite values.
Results may differ from the reference program's by a relative error of at most 0.0046.
Values may be sent and summed in bfloat16 or wider, within the bound.
No kernel may reach another device: no remote copies, remote signals or barrier semaphores. Data moves between devices by JAX's collectives and lax.ppermute only.
A program may use at most 192 MiB of HBM per device.

```python
import math
import jax
import jax.numpy as jnp
from jax import lax

NI = 320
NFACE = 5
FU = 80
K = 4
CAP = 8
REACH = 4
E_DEV = 16
NF = 400
CAPF = 9
OWNED = 40
ELEMS = 512
FACES = 1280
N_DOM = 16
N_SUB = 2


def handover_maps(key):
    devices = N_DOM * N_SUB
    entries = E_DEV * K
    offset_count = 2 * REACH + 1
    slot_total = offset_count * CAP
    base = jax.random.fold_in(key, 11)
    perm_key, count_key, pick_key = jax.random.split(base, 3)

    def one_choice(seed_key):
        score_key, lead_key = jax.random.split(seed_key)
        scores = jax.random.permutation(score_key, slot_total).astype(jnp.int32)
        leader = jax.random.randint(lead_key, (), 0, offset_count).astype(jnp.int32)
        block_of = jnp.arange(slot_total, dtype=jnp.int32) // CAP
        scores = scores - jnp.where(block_of == leader, slot_total, 0).astype(jnp.int32)
        order = jnp.argsort(scores, stable=True).astype(jnp.int32)
        return order[:entries]
    picked = jax.vmap(one_choice)(jax.random.split(perm_key, devices))
    counts = jax.random.randint(count_key, (devices, E_DEV), 1, K + 1).astype(jnp.int32)
    full_elements = (CAP + K - 1) // K
    counts = counts.at[:, :full_elements].set(K)
    is_live = (jnp.arange(K, dtype=jnp.int32)[None, None, :] < counts[:, :, None]).reshape(devices, entries)
    receiver = jnp.arange(devices, dtype=jnp.int32)[:, None]
    offset_row = picked // CAP
    column = picked % CAP
    source = (jnp.mod(receiver // N_SUB - offset_row + REACH, N_DOM) * N_SUB + receiver % N_SUB).astype(jnp.int32)
    recv_map = jnp.where(is_live, picked, -1).astype(jnp.int32).reshape(devices * E_DEV, K)
    element = jax.random.randint(pick_key, (devices, entries), 0, E_DEV).astype(jnp.int32)
    sender_map = jnp.full((devices, offset_count, CAP), -1, jnp.int32)
    sender_map = sender_map.at[source, offset_row, column].set(jnp.where(is_live, element, -1).astype(jnp.int32))
    return (sender_map, recv_map, counts.reshape(devices * E_DEV))


def face_maps(key):
    devices = N_DOM * N_SUB
    item_count = E_DEV * NFACE
    offset_count = 2 * REACH + 1
    base = jax.random.fold_in(key, 23)
    label_key, slot_key, row_key = jax.random.split(base, 3)
    labels = jax.random.permutation(label_key, item_count).astype(jnp.int32)
    shift_list = labels % offset_count - REACH
    slot_perm = jax.vmap(lambda seed_key: jax.random.permutation(seed_key, item_count).astype(jnp.int32))(jax.random.split(slot_key, devices))
    row_rank = jax.vmap(lambda seed_key: jax.random.permutation(seed_key, item_count).astype(jnp.int32))(jax.random.split(row_key, devices))
    shift_map = jax.vmap(lambda slots: jnp.zeros((item_count,), jnp.int32).at[slots].set(shift_list))(slot_perm)
    same = shift_list[:, None] == shift_list[None, :]
    earlier = slot_perm[:, None, :] < slot_perm[:, :, None]
    ranks = jnp.sum(jnp.where(same[None] & earlier, 1, 0), axis=2).astype(jnp.int32)
    device = jnp.arange(devices, dtype=jnp.int32)[:, None]
    owner = (device // N_SUB + shift_list[None, :]) % N_DOM * N_SUB + device % N_SUB
    labels_all = jnp.broadcast_to(jnp.arange(item_count, dtype=jnp.int32)[None, :], (devices, item_count))
    rows = row_rank[owner, labels_all] // 2
    shift_all = jnp.broadcast_to(shift_list[None, :] + REACH, (devices, item_count))
    row_map = jnp.full((devices, offset_count, CAPF), -1, jnp.int32)
    row_map = row_map.at[owner, shift_all, ranks].set(rows)
    return (shift_map.reshape(devices * E_DEV, NFACE), row_map)


def draw_send_elem(key, part):
    return handover_maps(key)[0]


def draw_recv_slot(key, part):
    return handover_maps(key)[1]


def draw_intersection_count(key, part):
    return handover_maps(key)[2]


def draw_face_shift(key, part):
    return face_maps(key)[0]


def draw_owner_row(key, part):
    return face_maps(key)[1]


def level_of(own_key, dims, cuts, least, largest):
    loudness = 1.0
    for dim, parts in cuts:
        draws = jax.random.uniform(jax.random.fold_in(jax.random.fold_in(own_key, 6), dim), (parts,), jnp.float32, least / len(cuts), largest / len(cuts))
        loudness = loudness * jnp.repeat(jnp.exp(draws), dims[dim] // parts).reshape((-1,) + (1,) * (len(dims) - 1 - dim))
    return loudness


def noise(key, dims, width, bound, pieces=(), held_as=jnp.bfloat16):
    array = jax.random.normal(key, dims, jnp.float32) * width
    if len(pieces) > 0:
        array = level_of(key, dims, pieces, -0.22, 0.18) * array
    return jnp.clip(array, min=-bound, max=bound).astype(held_as)


def setup_inputs(seed: int = 0) -> dict:
    keys = jax.random.split(jax.random.key(seed), 13)
    return {
        "old_states": noise(keys[0], (ELEMS, NI), 1.0, 6.0, ((0, 32),)),
        "send_elem": draw_send_elem(jax.random.fold_in(keys[12], 71), 0),
        "recv_slot": draw_recv_slot(jax.random.fold_in(keys[12], 71), 0),
        "intersection_count": draw_intersection_count(jax.random.fold_in(keys[12], 71), 0),
        "intersection_weight": jnp.clip(jnp.exp(math.log(1.0) - 2.3025851 * jax.random.uniform(keys[4], (ELEMS, K), jnp.float32) ** level_of(keys[4], (ELEMS, K), ((0, 32),), -0.2, 0.2)), 0.1, 1.0),
        "interior_inverse": noise(keys[5], (ELEMS, NI, NI), NI ** -0.5, 0.3125, ((0, 32),)),
        "inner_coupling": noise(keys[6], (ELEMS, NI, NF), 1.0, 6.0, ((0, 32),)),
        "face_coupling": noise(keys[7], (ELEMS, NF, NI), NI ** -0.5, 0.3125, ((0, 32),)),
        "face_mass": noise(keys[8], (FU, FU), 1.0, 6.0, (), jnp.float32),
        "face_scale": jnp.clip(jnp.exp(math.log(2.0) - 1.3862944 * jax.random.uniform(keys[9], (ELEMS, NFACE), jnp.float32) ** level_of(keys[9], (ELEMS, NFACE), ((0, 32),), -0.2, 0.2)), 0.5, 2.0),
        "face_shift": draw_face_shift(jax.random.fold_in(keys[12], 71), 0),
        "owner_row": draw_owner_row(jax.random.fold_in(keys[12], 71), 0),
    }


HIGH = lax.Precision.HIGHEST


def condense_block(element_block, face_mass):
    inverse, inner_part, outer_part, source, scales = element_block
    inverse32 = inverse.astype(jnp.float32)
    mapped = jnp.einsum("eab,ebc->eac", inverse32, inner_part.astype(jnp.float32), precision=HIGH).astype(jnp.bfloat16)
    interior_load = jnp.einsum("eab,eb->ea", inverse32, source.astype(jnp.float32), precision=HIGH).astype(jnp.bfloat16)
    rows_in = outer_part.reshape(outer_part.shape[0], NFACE, FU, NI).astype(jnp.float32)
    columns = mapped.reshape(mapped.shape[0], NI, NFACE, FU).astype(jnp.float32)
    correction = jnp.einsum("ejar,erjb->ejab", rows_in, columns, precision=HIGH)
    condensed = jnp.einsum("ejar,er->eja", rows_in, interior_load.astype(jnp.float32), precision=HIGH)
    schur_block = (scales[:, :, None, None] * face_mass[None, None] - correction).astype(jnp.bfloat16)
    right_side = (-condensed).astype(jnp.bfloat16)
    return jnp.concatenate([schur_block.reshape(schur_block.shape[0], NFACE, FU * FU), right_side], axis=2)


def reference(old_states, send_elem, recv_slot, intersection_count, intersection_weight, interior_inverse, inner_coupling, face_coupling, face_mass, face_scale, face_shift, owner_row):
    devices = N_DOM * N_SUB
    new_device = (jnp.arange(ELEMS) // E_DEV).astype(jnp.int32)
    new_dom = (new_device // N_SUB).astype(jnp.int32)
    new_sub = (new_device % N_SUB).astype(jnp.int32)
    safe_slot = jnp.maximum(recv_slot, 0).astype(jnp.int32)
    offset_row = safe_slot // CAP
    source_column = safe_slot % CAP
    source_device = (jnp.mod(new_dom[:, None] - offset_row + REACH, N_DOM) * N_SUB + new_sub[:, None]).astype(jnp.int32)
    local_element = send_elem[source_device, offset_row, source_column]
    old_index = (source_device * E_DEV + jnp.maximum(local_element, 0)).astype(jnp.int32)
    states = old_states[old_index].astype(jnp.float32)
    is_live = jnp.arange(K).astype(jnp.int32)[None, :] < intersection_count[:, None]
    weights = jnp.where(is_live, intersection_weight, jnp.zeros_like(intersection_weight))
    projected = (jnp.einsum("ek,ekr->er", weights, states, precision=HIGH) / jnp.sum(weights, axis=1, keepdims=True)).astype(jnp.bfloat16)

    def one_device(element_block):
        return condense_block(element_block, face_mass)

    blocks = (interior_inverse.reshape(devices, E_DEV, NI, NI), inner_coupling.reshape(devices, E_DEV, NI, NF), face_coupling.reshape(devices, E_DEV, NF, NI), projected.reshape(devices, E_DEV, NI), face_scale.reshape(devices, E_DEV, NFACE))
    payload = lax.map(one_device, blocks)

    item_count = E_DEV * NFACE
    shifts = face_shift.reshape(devices, item_count).astype(jnp.int32)
    order = jnp.arange(item_count).astype(jnp.int32)
    same = shifts[:, :, None] == shifts[:, None, :]
    before = order[None, None, :] < order[None, :, None]
    slot_rank = jnp.sum(jnp.where(same & before, 1, 0), axis=2).astype(jnp.int32)
    device = jnp.arange(devices).astype(jnp.int32)[:, None]
    owner = (jnp.mod(device // N_SUB + shifts, N_DOM) * N_SUB + device % N_SUB).astype(jnp.int32)
    owned_rows = owner_row[owner, shifts + REACH, slot_rank]
    face_index = (owner * OWNED + owned_rows).astype(jnp.int32)
    summed = jax.ops.segment_sum(payload.reshape(devices * item_count, FU * FU + FU).astype(jnp.float32), face_index.reshape(-1), num_segments=FACES)
    return summed[:, :FU * FU], summed[:, FU * FU:]
```

```python
import functools

import jax
import jax.numpy as jnp
from jax import lax
from jax.experimental import pallas as pl
from jax.experimental.pallas import tpu as pltpu
from jax.sharding import PartitionSpec as P

HIGH = lax.Precision.HIGHEST
LANES = 128
SUB = 8
NT = (((1,), (1,)), ((), ()))
TN = (((0,), (0,)), ((), ()))


def passed_along(block, axis, distance):
    size = lax.axis_size(axis)
    route = [((i - distance) % size, i) for i in range(size)]
    return lax.ppermute(block, axis, route)


def pack_states_kernel(devices, send_ref, old_ref, out_ref, src, buf):
    slots, offsets = send_ref.shape
    reach = (offsets - 1) // 2
    me = lax.axis_index("dom")
    src[...] = old_ref[...].astype(jnp.float32)
    buf[...] = jnp.zeros_like(buf)
    for t in range(offsets):
        target = lax.rem(me + (t - reach + devices), devices)
        for c in range(slots):
            element = jnp.maximum(send_ref[c, t], 0)
            buf[target, pl.ds(c, 1), :] = src[pl.ds(element, 1), :]
    out_ref[...] = buf[...].astype(jnp.bfloat16)


def condense_kernel(
    devices,
    dims,
    shift_ref,
    scale_ref,
    states_ref,
    recv_ref,
    count_ref,
    weight_ref,
    mass_ref,
    inverse_hbm,
    inner_hbm,
    face_hbm,
    *refs,
):
    elements, faces, unknowns, interior, offsets, ranks, slots = dims
    outs = refs[:offsets]
    (left, inverse, rows, mapped, mass, square, flat, slot_item, slot_scale, used,
     left_sem, inverse_sem, rows_sem) = refs[offsets:]
    reach = (offsets - 1) // 2
    nf = faces * unknowns
    extra = left.shape[1] - nf
    chunk = unknowns // SUB

    def copies(e):
        return (
            pltpu.make_async_copy(inverse_hbm.at[e], inverse.at[e], inverse_sem.at[e]),
            pltpu.make_async_copy(inner_hbm.at[e], left.at[e, pl.ds(0, nf)], left_sem.at[e]),
        )

    for e in range(elements):
        for copy in copies(e):
            copy.start()
    rows_copy = pltpu.make_async_copy(face_hbm, rows, rows_sem)
    rows_copy.start()

    mass[...] = jnp.zeros_like(mass)
    mass[:, :unknowns] = mass_ref[...]

    me = lax.axis_index("dom")
    slot = recv_ref[...]
    live = lax.broadcasted_iota(jnp.int32, slot.shape, 0) < count_ref[...]
    weights = jnp.where(live, weight_ref[...], 0.0)
    weights = weights / jnp.sum(weights, axis=0, keepdims=True)
    slot = jnp.maximum(slot, 0)
    source = lax.rem(me - slot // slots + (reach + devices), devices)
    place = source * slots + slot % slots
    total = states_ref.shape[0]
    row = lax.broadcasted_iota(jnp.int32, (total, elements), 0)
    mix = jnp.zeros((total, elements), jnp.float32)
    for k in range(slot.shape[0]):
        mix = mix + jnp.where(row == place[k : k + 1, :], weights[k : k + 1, :], 0.0)
    projected = lax.dot_general(
        mix, states_ref[...].astype(jnp.float32), TN, precision=HIGH,
        preferred_element_type=jnp.float32,
    ).astype(jnp.bfloat16)
    for e in range(elements):
        left[e, pl.ds(nf, extra), :] = jnp.broadcast_to(projected[e : e + 1, :], (extra, interior))

    for t in range(offsets):
        used[t] = 0
    for s in range(offsets * ranks):
        slot_item[s] = 0
        slot_scale[s] = 1.0

    def map_element(e, carry):
        for copy in copies(e):
            copy.wait()
        product = lax.dot_general(
            left[e], inverse[e], NT, preferred_element_type=jnp.float32
        ).astype(jnp.bfloat16)
        tail = product[nf:, :]
        for j in range(faces):
            item = e * faces + j
            mapped[item, pl.ds(0, unknowns), :] = product[j * unknowns : (j + 1) * unknowns, :]
            for start in range(unknowns, mapped.shape[1], extra):
                mapped[item, pl.ds(start, extra), :] = tail
            shift = shift_ref[j, e] + reach
            rank = used[shift]
            used[shift] = rank + 1
            slot_item[shift * ranks + rank] = item
            slot_scale[shift * ranks + rank] = scale_ref[j, e]
        return carry

    lax.fori_loop(0, elements, map_element, 0)
    rows_copy.wait()

    lane = lax.broadcasted_iota(jnp.int32, (SUB, LANES), 1)
    tiles = flat.shape[2] // LANES
    for t in range(offsets):
        for k in range(ranks):
            s = t * ranks + k
            item = slot_item[s]
            product = lax.dot_general(
                rows[item], mapped[item], NT, preferred_element_type=jnp.float32
            )
            square[k] = slot_scale[s] * mass[...] - product
            parts = [square[k, pl.ds(g, SUB, stride=chunk), :] for g in range(chunk)]
            turned = [
                p if (g * unknowns) % LANES == 0 else pltpu.roll(p, (g * unknowns) % LANES, 1)
                for g, p in enumerate(parts)
            ]
            for i in range(tiles):
                low = i * LANES
                first = low // unknowns
                if first < chunk:
                    value = turned[first]
                    for g in range(first + 1, min(chunk, -(-(low + LANES) // unknowns))):
                        value = jnp.where(lane >= g * unknowns - low, turned[g], value)
                if i == tiles - 1:
                    for g in range(chunk):
                        value = jnp.where(lane == unknowns + g, parts[g], value)
                flat[k, :, pl.ds(low, LANES)] = value
        outs[t][...] = flat[...].astype(jnp.bfloat16)


def assemble_kernel(dims, owner_ref, *refs):
    owned, unknowns, offsets, ranks = dims
    pieces = refs[:offsets]
    schur_ref, rhs_ref, total = refs[offsets:]
    chunk = unknowns // SUB
    width = chunk * unknowns
    last = total.shape[2] - LANES
    total[...] = jnp.zeros_like(total)
    for t in range(offsets):
        for k in range(ranks):
            row = owner_ref[t, k]
            row = jnp.where(row < 0, owned, row)
            total[row] = total[row] + pieces[t][k].astype(jnp.float32)
    for group in range(owned // SUB):
        faces = pl.ds(group * SUB, SUB)
        for a in range(SUB):
            value = total[faces, a, :]
            schur_ref[faces, a * width : (a + 1) * width] = value[:, :width]
            rhs_ref[faces, a * chunk : (a + 1) * chunk] = value[
                :, last + unknowns : last + unknowns + chunk
            ]


def per_device(
    old_states,
    send_elem,
    recv_slot,
    intersection_count,
    intersection_weight,
    interior_inverse,
    inner_coupling,
    face_coupling,
    face_mass,
    face_scale,
    face_shift,
    owner_row,
):
    devices = lax.axis_size("dom")
    offsets, slots = send_elem.shape[1:]
    reach = (offsets - 1) // 2
    ranks = owner_row.shape[2]
    elements, interior = old_states.shape
    faces = face_scale.shape[1]
    unknowns = face_mass.shape[0]
    nf = faces * unknowns
    items = elements * faces
    owned = items // 2
    width = -(-(unknowns // SUB * unknowns) // LANES) * LANES
    smem = pl.BlockSpec(memory_space=pltpu.SMEM)
    vmem = pl.BlockSpec(memory_space=pltpu.VMEM)
    anywhere = pl.BlockSpec(memory_space=pl.ANY)
    bf16, f32 = jnp.bfloat16, jnp.float32

    outgoing = pl.pallas_call(
        functools.partial(pack_states_kernel, devices),
        out_shape=jax.ShapeDtypeStruct((devices, slots, interior), bf16),
        in_specs=[smem, vmem],
        out_specs=vmem,
        scratch_shapes=[
            pltpu.VMEM((elements, interior), f32),
            pltpu.VMEM((devices, slots, interior), f32),
        ],
        name="pack_states",
    )(send_elem[0].T, old_states)
    states = lax.all_to_all(outgoing, "dom", 0, 0)

    dims = (elements, faces, unknowns, interior, offsets, ranks, slots)
    extra = 16
    packed = pl.pallas_call(
        functools.partial(condense_kernel, devices, dims),
        out_shape=[jax.ShapeDtypeStruct((ranks, SUB, width), bf16)] * offsets,
        in_specs=[smem, smem] + [vmem] * 5 + [anywhere] * 3,
        out_specs=[vmem] * offsets,
        scratch_shapes=[
            pltpu.VMEM((elements, nf + extra, interior), bf16),
            pltpu.VMEM((elements, interior, interior), bf16),
            pltpu.VMEM((items, unknowns, interior), bf16),
            pltpu.VMEM((items, LANES, interior), bf16),
            pltpu.VMEM((unknowns, LANES), f32),
            pltpu.VMEM((ranks, unknowns, LANES), f32),
            pltpu.VMEM((ranks, SUB, width), f32),
            pltpu.SMEM((offsets * ranks,), jnp.int32),
            pltpu.SMEM((offsets * ranks,), f32),
            pltpu.SMEM((offsets,), jnp.int32),
            pltpu.SemaphoreType.DMA((elements,)),
            pltpu.SemaphoreType.DMA((elements,)),
            pltpu.SemaphoreType.DMA,
        ],
        compiler_params=pltpu.CompilerParams(vmem_limit_bytes=40 * 2**20),
        name="condense",
    )(
        face_shift.T,
        face_scale.T,
        states.reshape(devices * slots, interior),
        recv_slot.T,
        intersection_count.reshape(1, elements),
        intersection_weight.T,
        face_mass,
        interior_inverse,
        jnp.swapaxes(inner_coupling, 1, 2),
        face_coupling.reshape(items, unknowns, interior),
    )

    order = sorted(range(offsets), key=lambda t: (t > reach, -abs(t - reach)))
    pieces = list(packed)
    for t in order:
        if t != reach:
            pieces[t] = passed_along(packed[t], "dom", t - reach)

    schur, rhs = pl.pallas_call(
        functools.partial(assemble_kernel, (owned, unknowns, offsets, ranks)),
        out_shape=[
            jax.ShapeDtypeStruct((owned, unknowns * unknowns), f32),
            jax.ShapeDtypeStruct((owned, unknowns), f32),
        ],
        in_specs=[smem] + [vmem] * offsets,
        out_specs=[vmem, vmem],
        scratch_shapes=[pltpu.VMEM((owned + 1, SUB, width), f32)],
        name="assemble",
    )(owner_row[0], *pieces)
    return schur, rhs


def solution(mesh):
    in_specs = (
        P(("dom", "sub"), None),
        P(("dom", "sub"), None, None),
        P(("dom", "sub"), None),
        P(("dom", "sub")),
        P(("dom", "sub"), None),
        P(("dom", "sub"), None, None),
        P(("dom", "sub"), None, None),
        P(("dom", "sub"), None, None),
        P(),
        P(("dom", "sub"), None),
        P(("dom", "sub"), None),
        P(("dom", "sub"), None, None),
    )
    out_specs = (P(("dom", "sub"), None), P(("dom", "sub"), None))
    return jax.shard_map(
        per_device, mesh=mesh, in_specs=in_specs, out_specs=out_specs, check_vma=False
    )
```

```python
import functools

import jax
import jax.numpy as jnp
from jax import lax
from jax.experimental import pallas as pl
from jax.experimental.pallas import tpu as pltpu
from jax.sharding import PartitionSpec as P

HIGH = lax.Precision.HIGHEST
LANES = 128
SUB = 8
VMEM_BYTES = 67_043_328
AHEAD = 6
UNROLL = 2
EXTRA = 16
NN = (((1,), (0,)), ((), ()))
NT = (((1,), (1,)), ((), ()))
TN = (((0,), (0,)), ((), ()))


def passed_along(block, axis, distance):
    size = lax.axis_size(axis)
    route = [((i - distance) % size, i) for i in range(size)]
    return lax.ppermute(block, axis, route)


def pack_states_kernel(devices, send_hbm, old_hbm, out_ref, send, old, src, buf, sems):
    slots, offsets = send.shape
    reach = (offsets - 1) // 2
    loads = fetch((send_hbm, send), (old_hbm, old), sems=sems)
    me = lax.axis_index("dom")
    buf[...] = jnp.zeros_like(buf)
    for load in loads:
        load.wait()
    src[...] = old[...].astype(jnp.float32)
    for t in range(offsets):
        target = lax.rem(me + (t - reach + devices), devices)
        for c in range(slots):
            element = jnp.maximum(send[c, t], 0)
            buf[target, pl.ds(c, 1), :] = src[pl.ds(element, 1), :]
    out_ref[...] = buf[...].astype(jnp.bfloat16)


def tile_plan(unknowns, ranks):
    full, rest = divmod(unknowns // SUB * unknowns, LANES)
    share = LANES // rest
    return full, rest, share, -(-ranks // share)


def rest_start(unknowns, ranks):
    _, rest, share, sides = tile_plan(unknowns, ranks)
    start = rest * (ranks - share * (sides - 1))
    assert start + unknowns // SUB * ranks <= LANES
    return start


def in_hbm(array):
    return pltpu.with_memory_space_constraint(array, pltpu.HBM)


def fetch(*pairs, sems):
    loads = [
        pltpu.make_async_copy(source, target, sems.at[i])
        for i, (source, target) in enumerate(pairs)
    ]
    for load in loads:
        load.start()
    return loads


def condense_kernel(
    devices,
    dims,
    states_ref,
    shift_hbm,
    scale_hbm,
    recv_hbm,
    count_hbm,
    weight_hbm,
    mass_hbm,
    face_hbm,
    inverse_hbm,
    inner_hbm,
    *refs,
):
    elements, faces, unknowns, interior, offsets, ranks, slots = dims
    outs = refs[:offsets]
    (shift_ref, scale_ref, recv, count, weight, mass_in, rows, inverse, inner, tail, mass,
     square, packed, side, used, small_sem, sems) = refs[offsets:]
    reach = (offsets - 1) // 2
    chunk = unknowns // SUB
    full, rest, share, sides = tile_plan(unknowns, ranks)
    ahead = min(AHEAD, elements)

    def loads(e):
        return (
            pltpu.make_async_copy(inverse_hbm.at[e], inverse.at[e], sems.at[0, e]),
            pltpu.make_async_copy(face_hbm.at[e], rows.at[e], sems.at[1, e]),
            pltpu.make_async_copy(inner_hbm.at[e], inner.at[e], sems.at[2, e]),
        )

    def start(e):
        for load in loads(e):
            load.start()

    small = fetch(
        (shift_hbm, shift_ref), (scale_hbm, scale_ref), (recv_hbm, recv), (count_hbm, count),
        (weight_hbm, weight), (mass_hbm, mass_in), sems=small_sem,
    )
    for e in range(ahead):
        start(e)
    for t in range(offsets):
        used[t] = 0
    packed[...] = jnp.zeros_like(packed)
    side[...] = jnp.zeros_like(side)
    mass[...] = jnp.zeros_like(mass)
    for load in small:
        load.wait()
    mass[:, :unknowns] = mass_in[...]

    me = lax.axis_index("dom")
    slot = recv[...]
    live = lax.broadcasted_iota(jnp.int32, slot.shape, 0) < count[...]
    weights = jnp.where(live, weight[...], 0.0)
    weights = weights / jnp.sum(weights, axis=0, keepdims=True)
    slot = jnp.maximum(slot, 0)
    source = lax.rem(me - slot // slots + (reach + devices), devices)
    place = source * slots + slot % slots
    total = states_ref.shape[0]
    row = lax.broadcasted_iota(jnp.int32, (total, elements), 0)
    mix = jnp.zeros((total, elements), jnp.float32)
    for k in range(slot.shape[0]):
        mix = mix + jnp.where(row == place[k : k + 1, :], weights[k : k + 1, :], 0.0)
    projected = lax.dot_general(
        mix, states_ref[...].astype(jnp.float32), TN, precision=HIGH,
        preferred_element_type=jnp.float32,
    ).astype(jnp.bfloat16)
    for e in range(elements):
        tail[e] = jnp.broadcast_to(projected[e : e + 1, :], tail.shape[1:])

    lane = lax.broadcasted_iota(jnp.int32, (SUB, LANES), 1)

    def condense_element(e, carry):
        for load in loads(e):
            load.wait()

        @pl.when(e + ahead < elements)
        def _():
            start(e + ahead)

        product = lax.dot_general(
            rows[e], inverse[e], NN, preferred_element_type=jnp.float32
        ).astype(jnp.bfloat16)
        for j in range(faces):
            shift = shift_ref[j, e] + reach
            rank = used[shift]
            used[shift] = rank + 1
            spot = (shift * ranks + rank) * full
            correction = lax.dot_general(
                product[j * unknowns : (j + 1) * unknowns, :],
                jnp.concatenate([inner[e, j], tail[e]], axis=0),
                NT,
                preferred_element_type=jnp.float32,
            )
            square[j, :, pl.ds(0, mass.shape[1])] = scale_ref[j, e] * mass[...] - correction
            parts = [square[j, pl.ds(g, SUB, stride=chunk), :] for g in range(chunk)]
            turned = [
                p if (g * unknowns) % LANES == 0 else pltpu.roll(p, (g * unknowns) % LANES, 1)
                for g, p in enumerate(parts)
            ]
            for i in range(full + 1):
                low = i * LANES
                first = low // unknowns
                value = turned[first]
                for g in range(first + 1, min(chunk, -(-(low + LANES) // unknowns))):
                    value = jnp.where(lane >= g * unknowns - low, turned[g], value)
                if i < full:
                    packed[spot + i] = value.astype(packed.dtype)
            value = jnp.where(lane < rest, value, 0.0)
            spot = shift * sides + rank // share
            side[spot] = side[spot] + pltpu.roll(value, rest * (rank % share), 1)
            value = jnp.zeros_like(value)
            for g in range(chunk):
                value = jnp.where(lane == unknowns + g, parts[g], value)
            spot = shift * sides + (sides - 1)
            turn = (rest_start(unknowns, ranks) - unknowns) % LANES
            side[spot] = side[spot] + pltpu.roll(value, lax.rem(turn + chunk * rank, LANES), 1)
        return carry

    lax.fori_loop(0, elements, condense_element, 0, unroll=UNROLL)
    for t in range(offsets):
        outs[t][pl.ds(0, ranks * full)] = packed[pl.ds(t * ranks * full, ranks * full)]
        outs[t][pl.ds(ranks * full, sides)] = side[pl.ds(t * sides, sides)].astype(jnp.bfloat16)


def assemble_kernel(dims, owner_hbm, *refs):
    owned, unknowns, offsets, ranks = dims
    pieces = refs[:offsets]
    schur_ref, rhs_ref, owner, total, sems = refs[offsets:]
    chunk = unknowns // SUB
    width = chunk * unknowns
    full, rest, share, sides = tile_plan(unknowns, ranks)
    last = full * LANES
    lane = lax.broadcasted_iota(jnp.int32, (SUB, LANES), 1)
    loads = fetch((owner_hbm, owner), sems=sems)
    total[...] = jnp.zeros_like(total)
    loads[0].wait()
    for t in range(offsets):
        ends = [pieces[t][ranks * full + i].astype(jnp.float32) for i in range(sides)]
        for k in range(ranks):
            row = owner[t, 0, k]
            row = jnp.where(row < 0, owned, row)
            for i in range(full):
                tile = pl.ds(i * LANES, LANES)
                total[row, :, tile] = total[row, :, tile] + pieces[t][k * full + i].astype(jnp.float32)
            tail = pltpu.roll(ends[-1], (unknowns - rest_start(unknowns, ranks) - chunk * k) % LANES, 1)
            turn = -rest * (k % share) % LANES
            end = ends[k // share]
            tail = jnp.where(lane < rest, pltpu.roll(end, turn, 1) if turn else end, tail)
            total[row, :, pl.ds(last, LANES)] = total[row, :, pl.ds(last, LANES)] + tail
    for group in range(owned // SUB):
        faces = pl.ds(group * SUB, SUB)
        for a in range(SUB):
            value = total[faces, a, :]
            schur_ref[faces, a * width : (a + 1) * width] = value[:, :width]
            rhs_ref[faces, a * chunk : (a + 1) * chunk] = value[
                :, last + unknowns : last + unknowns + chunk
            ]


def per_device(
    old_states,
    send_elem,
    recv_slot,
    intersection_count,
    intersection_weight,
    interior_inverse,
    inner_coupling,
    face_coupling,
    face_mass,
    face_scale,
    face_shift,
    owner_row,
):
    devices = lax.axis_size("dom")
    offsets, slots = send_elem.shape[1:]
    reach = (offsets - 1) // 2
    ranks = owner_row.shape[2]
    elements, interior = old_states.shape
    neighbours = recv_slot.shape[1]
    faces = face_scale.shape[1]
    unknowns = face_mass.shape[0]
    nf = faces * unknowns
    items = elements * faces
    owned = items // 2
    full, rest, share, sides = tile_plan(unknowns, ranks)
    width = (full + 1) * LANES
    vmem = pl.BlockSpec(memory_space=pltpu.VMEM)
    hbm = pl.BlockSpec(memory_space=pltpu.HBM)
    bf16, f32 = jnp.bfloat16, jnp.float32

    outgoing = pl.pallas_call(
        functools.partial(pack_states_kernel, devices),
        out_shape=jax.ShapeDtypeStruct((devices, slots, interior), bf16),
        in_specs=[hbm, hbm],
        out_specs=vmem,
        scratch_shapes=[
            pltpu.SMEM((slots, offsets), jnp.int32),
            pltpu.VMEM((elements, interior), bf16),
            pltpu.VMEM((elements, interior), f32),
            pltpu.VMEM((devices, slots, interior), f32),
            pltpu.SemaphoreType.DMA((2,)),
        ],
        compiler_params=pltpu.CompilerParams(vmem_limit_bytes=16 * 2**20),
        name="pack_states",
    )(in_hbm(send_elem[0].T), in_hbm(old_states))
    states = lax.all_to_all(outgoing, "dom", 0, 0)

    dims = (elements, faces, unknowns, interior, offsets, ranks, slots)
    by_face = (elements, faces, unknowns, interior)
    packed = pl.pallas_call(
        functools.partial(condense_kernel, devices, dims),
        out_shape=[jax.ShapeDtypeStruct((ranks * full + sides, SUB, LANES), bf16)] * offsets,
        in_specs=[vmem] + [hbm] * 9,
        out_specs=[vmem] * offsets,
        scratch_shapes=[
            pltpu.SMEM((faces, elements), jnp.int32),
            pltpu.SMEM((faces, elements), f32),
            pltpu.VMEM((neighbours, elements), jnp.int32),
            pltpu.VMEM((1, elements), jnp.int32),
            pltpu.VMEM((neighbours, elements), f32),
            pltpu.VMEM((unknowns, unknowns), f32),
            pltpu.VMEM((elements, nf, interior), bf16),
            pltpu.VMEM((elements, interior, interior), bf16),
            pltpu.VMEM(by_face, bf16),
            pltpu.VMEM((elements, EXTRA, interior), bf16),
            pltpu.VMEM((unknowns, unknowns + EXTRA), f32),
            pltpu.VMEM((faces, unknowns, LANES), f32),
            pltpu.VMEM((offsets * ranks * full, SUB, LANES), bf16),
            pltpu.VMEM((offsets * sides, SUB, LANES), f32),
            pltpu.SMEM((offsets,), jnp.int32),
            pltpu.SemaphoreType.DMA((6,)),
            pltpu.SemaphoreType.DMA((3, elements)),
        ],
        cost_estimate=pl.CostEstimate(
            flops=2 * items * unknowns * unknowns * interior,
            bytes_accessed=2 * items * interior * 3 * unknowns,
            transcendentals=0,
        ),
        compiler_params=pltpu.CompilerParams(vmem_limit_bytes=50 * 2**20),
        name="condense",
    )(
        states.reshape(devices * slots, interior),
        in_hbm(face_shift.T),
        in_hbm(face_scale.T),
        in_hbm(recv_slot.T),
        in_hbm(intersection_count.reshape(1, elements)),
        in_hbm(intersection_weight.T),
        in_hbm(face_mass),
        in_hbm(face_coupling),
        in_hbm(interior_inverse),
        in_hbm(jnp.swapaxes(inner_coupling, 1, 2).reshape(by_face)),
    )

    order = sorted(range(offsets), key=lambda t: (t > reach, -abs(t - reach)))
    pieces = list(packed)
    for t in order:
        if t != reach:
            pieces[t] = passed_along(packed[t], "dom", t - reach)

    schur, rhs = pl.pallas_call(
        functools.partial(assemble_kernel, (owned, unknowns, offsets, ranks)),
        out_shape=[
            jax.ShapeDtypeStruct((owned, unknowns * unknowns), f32),
            jax.ShapeDtypeStruct((owned, unknowns), f32),
        ],
        in_specs=[hbm] + [vmem] * offsets,
        out_specs=[vmem, vmem],
        scratch_shapes=[
            pltpu.SMEM((offsets, 1, ranks), jnp.int32),
            pltpu.VMEM((owned + 1, SUB, width), f32),
            pltpu.SemaphoreType.DMA((1,)),
        ],
        compiler_params=pltpu.CompilerParams(vmem_limit_bytes=16 * 2**20),
        name="assemble",
    )(in_hbm(jnp.swapaxes(owner_row, 0, 1)), *pieces)
    return schur, rhs


def solution(mesh):
    in_specs = (
        P(("dom", "sub"), None),
        P(("dom", "sub"), None, None),
        P(("dom", "sub"), None),
        P(("dom", "sub")),
        P(("dom", "sub"), None),
        P(("dom", "sub"), None, None),
        P(("dom", "sub"), None, None),
        P(("dom", "sub"), None, None),
        P(),
        P(("dom", "sub"), None),
        P(("dom", "sub"), None),
        P(("dom", "sub"), None, None),
    )
    out_specs = (P(("dom", "sub"), None), P(("dom", "sub"), None))
    return jax.shard_map(
        per_device, mesh=mesh, in_specs=in_specs, out_specs=out_specs, check_vma=False
    )
```

```python
import functools

import jax
import jax.numpy as jnp
from jax import lax
from jax.experimental import pallas as pl
from jax.experimental.pallas import tpu as pltpu
from jax.sharding import PartitionSpec as P

HIGH = lax.Precision.HIGHEST
LANES = 128
SUB = 8
VMEM_BYTES = 67_043_328
AHEAD = 2
GROUP = 4
EXTRA = 16
NN = (((1,), (0,)), ((), ()))
NT = (((1,), (1,)), ((), ()))
TN = (((0,), (0,)), ((), ()))


def passed_along(block, axis, distance):
    size = lax.axis_size(axis)
    route = [((i - distance) % size, i) for i in range(size)]
    return lax.ppermute(block, axis, route)


def pack_states_kernel(devices, send_hbm, old_hbm, out_ref, send, old, src, buf, sems):
    slots, offsets = send.shape
    reach = (offsets - 1) // 2
    loads = fetch((send_hbm, send), (old_hbm, old), sems=sems)
    me = lax.axis_index("dom")
    buf[...] = jnp.zeros_like(buf)
    for load in loads:
        load.wait()
    src[...] = old[...].astype(jnp.float32)
    for t in range(offsets):
        target = lax.rem(me + (t - reach + devices), devices)
        for c in range(slots):
            element = jnp.maximum(send[c, t], 0)
            buf[target, pl.ds(c, 1), :] = src[pl.ds(element, 1), :]
    out_ref[...] = buf[...].astype(jnp.bfloat16)


def tile_plan(unknowns, ranks):
    full, rest = divmod(unknowns // SUB * unknowns, LANES)
    share = LANES // rest
    return full, rest, share, -(-ranks // share)


def rest_start(unknowns, ranks):
    _, rest, share, sides = tile_plan(unknowns, ranks)
    start = rest * (ranks - share * (sides - 1))
    assert start + unknowns // SUB * ranks <= LANES
    return start


def in_hbm(array):
    return pltpu.with_memory_space_constraint(array, pltpu.HBM)


def fetch(*pairs, sems):
    loads = [
        pltpu.make_async_copy(source, target, sems.at[i])
        for i, (source, target) in enumerate(pairs)
    ]
    for load in loads:
        load.start()
    return loads


def condense_kernel(
    devices,
    dims,
    states_ref,
    shift_hbm,
    scale_hbm,
    recv_hbm,
    count_hbm,
    weight_hbm,
    mass_hbm,
    face_hbm,
    inverse_hbm,
    inner_hbm,
    *refs,
):
    elements, faces, unknowns, interior, offsets, ranks, slots = dims
    outs = refs[:offsets]
    (shift_ref, scale_ref, recv, count, weight, mass_in, rows, inverse, inner, product, tail, mass,
     square, slot_item, slot_scale, used, small_sem, sems) = refs[offsets:]
    reach = (offsets - 1) // 2
    chunk = unknowns // SUB
    full, rest, share, sides = tile_plan(unknowns, ranks)
    groups = elements // GROUP

    def part(ref, group):
        return ref.at[pl.ds(group * GROUP, GROUP)]

    def loads(group):
        return (
            pltpu.make_async_copy(part(inverse_hbm, group), part(inverse, group), sems.at[0, group]),
            pltpu.make_async_copy(part(face_hbm, group), part(rows, group), sems.at[1, group]),
        )

    def inner_load(group):
        return pltpu.make_async_copy(part(inner_hbm, group), part(inner, group), sems.at[2, group])

    def start(group):
        for load in loads(group):
            load.start()

    small = fetch(
        (shift_hbm, shift_ref), (scale_hbm, scale_ref), (recv_hbm, recv), (count_hbm, count),
        (weight_hbm, weight), (mass_hbm, mass_in), sems=small_sem,
    )
    for group in range(AHEAD):
        start(group)
    for t in range(offsets):
        used[t] = 0
    for s in range(offsets * ranks):
        slot_item[s] = 0
        slot_scale[s] = 1.0
    mass[...] = jnp.zeros_like(mass)
    for load in small:
        load.wait()
    mass[:, :unknowns] = mass_in[...]

    me = lax.axis_index("dom")
    slot = recv[...]
    live = lax.broadcasted_iota(jnp.int32, slot.shape, 0) < count[...]
    weights = jnp.where(live, weight[...], 0.0)
    weights = weights / jnp.sum(weights, axis=0, keepdims=True)
    slot = jnp.maximum(slot, 0)
    source = lax.rem(me - slot // slots + (reach + devices), devices)
    place = source * slots + slot % slots
    total = states_ref.shape[0]
    row = lax.broadcasted_iota(jnp.int32, (total, elements), 0)
    mix = jnp.zeros((total, elements), jnp.float32)
    for k in range(slot.shape[0]):
        mix = mix + jnp.where(row == place[k : k + 1, :], weights[k : k + 1, :], 0.0)
    projected = lax.dot_general(
        mix, states_ref[...].astype(jnp.float32), TN, precision=HIGH,
        preferred_element_type=jnp.float32,
    ).astype(jnp.bfloat16)
    for e in range(elements):
        tail[e] = jnp.broadcast_to(projected[e : e + 1, :], tail.shape[1:])

    def product_group(group, carry):
        for load in loads(group):
            load.wait()

        @pl.when(group + AHEAD < groups)
        def _():
            start(group + AHEAD)

        inner_load(group).start()

        for i in range(GROUP):
            e = group * GROUP + i
            block = lax.dot_general(
                rows[e], inverse[e], NN, preferred_element_type=jnp.float32
            ).astype(jnp.bfloat16)
            for j in range(faces):
                item = e * faces + j
                product[item] = block[j * unknowns : (j + 1) * unknowns, :]
                shift = shift_ref[j, e] + reach
                rank = used[shift]
                used[shift] = rank + 1
                slot_item[shift * ranks + rank] = item
                slot_scale[shift * ranks + rank] = scale_ref[j, e]
        return carry

    lax.fori_loop(0, groups, product_group, 0)
    for group in range(groups):
        inner_load(group).wait()

    lane = lax.broadcasted_iota(jnp.int32, (SUB, LANES), 1)
    turn = rest_start(unknowns, ranks) - unknowns
    for t in range(offsets):
        ends = [jnp.zeros((SUB, LANES), jnp.float32)] * sides
        for k in range(ranks):
            s = t * ranks + k
            item = slot_item[s]
            element = item // faces
            correction = lax.dot_general(
                product[item],
                jnp.concatenate([inner[element, item % faces], tail[element]], axis=0),
                NT,
                preferred_element_type=jnp.float32,
            )
            spot = s % square.shape[0]
            square[spot, :, pl.ds(0, mass.shape[1])] = slot_scale[s] * mass[...] - correction
            parts = [square[spot, pl.ds(g, SUB, stride=chunk), :] for g in range(chunk)]
            turned = [turn_lanes(p, g * unknowns) for g, p in enumerate(parts)]
            for i in range(full):
                low = i * LANES
                first = low // unknowns
                value = turned[first]
                for g in range(first + 1, min(chunk, -(-(low + LANES) // unknowns))):
                    value = jnp.where(lane >= g * unknowns - low, turned[g], value)
                outs[t][k * full + i] = value.astype(jnp.bfloat16)
            low = rest * (k % share)
            value = turn_lanes(parts[-1], (chunk - 1) * unknowns - full * LANES + low)
            inside = (lane >= low) & (lane < low + rest)
            ends[k // share] = jnp.where(inside, value, ends[k // share])
            value = jnp.zeros_like(value)
            for g in range(chunk):
                value = jnp.where(lane == unknowns + g, parts[g], value)
            ends[-1] = ends[-1] + turn_lanes(value, turn + chunk * k)
        for i in range(sides):
            outs[t][ranks * full + i] = ends[i].astype(jnp.bfloat16)


def turn_lanes(value, amount):
    amount = amount % LANES
    return pltpu.roll(value, amount, 1) if amount else value


def assemble_kernel(dims, owner_hbm, *refs):
    owned, unknowns, offsets, ranks = dims
    pieces = refs[:offsets]
    schur_ref, rhs_ref, owner, total, sems = refs[offsets:]
    chunk = unknowns // SUB
    width = chunk * unknowns
    full, rest, share, sides = tile_plan(unknowns, ranks)
    last = full * LANES
    lane = lax.broadcasted_iota(jnp.int32, (SUB, LANES), 1)
    loads = fetch((owner_hbm, owner), sems=sems)
    total[...] = jnp.zeros_like(total)
    loads[0].wait()
    for t in range(offsets):
        ends = [pieces[t][ranks * full + i].astype(jnp.float32) for i in range(sides)]
        for k in range(ranks):
            row = owner[t, 0, k]
            row = jnp.where(row < 0, owned, row)
            for i in range(full):
                tile = pl.ds(i * LANES, LANES)
                total[row, :, tile] = total[row, :, tile] + pieces[t][k * full + i].astype(jnp.float32)
            tail = pltpu.roll(ends[-1], (unknowns - rest_start(unknowns, ranks) - chunk * k) % LANES, 1)
            turn = -rest * (k % share) % LANES
            end = ends[k // share]
            tail = jnp.where(lane < rest, pltpu.roll(end, turn, 1) if turn else end, tail)
            total[row, :, pl.ds(last, LANES)] = total[row, :, pl.ds(last, LANES)] + tail
    for group in range(owned // SUB):
        faces = pl.ds(group * SUB, SUB)
        for a in range(SUB):
            value = total[faces, a, :]
            schur_ref[faces, a * width : (a + 1) * width] = value[:, :width]
            rhs_ref[faces, a * chunk : (a + 1) * chunk] = value[
                :, last + unknowns : last + unknowns + chunk
            ]


def per_device(
    old_states,
    send_elem,
    recv_slot,
    intersection_count,
    intersection_weight,
    interior_inverse,
    inner_coupling,
    face_coupling,
    face_mass,
    face_scale,
    face_shift,
    owner_row,
):
    devices = lax.axis_size("dom")
    offsets, slots = send_elem.shape[1:]
    reach = (offsets - 1) // 2
    ranks = owner_row.shape[2]
    elements, interior = old_states.shape
    neighbours = recv_slot.shape[1]
    faces = face_scale.shape[1]
    unknowns = face_mass.shape[0]
    nf = faces * unknowns
    items = elements * faces
    owned = items // 2
    full, rest, share, sides = tile_plan(unknowns, ranks)
    width = (full + 1) * LANES
    vmem = pl.BlockSpec(memory_space=pltpu.VMEM)
    hbm = pl.BlockSpec(memory_space=pltpu.HBM)
    bf16, f32 = jnp.bfloat16, jnp.float32

    outgoing = pl.pallas_call(
        functools.partial(pack_states_kernel, devices),
        out_shape=jax.ShapeDtypeStruct((devices, slots, interior), bf16),
        in_specs=[hbm, hbm],
        out_specs=vmem,
        scratch_shapes=[
            pltpu.SMEM((slots, offsets), jnp.int32),
            pltpu.VMEM((elements, interior), bf16),
            pltpu.VMEM((elements, interior), f32),
            pltpu.VMEM((devices, slots, interior), f32),
            pltpu.SemaphoreType.DMA((2,)),
        ],
        compiler_params=pltpu.CompilerParams(vmem_limit_bytes=16 * 2**20),
        name="pack_states",
    )(in_hbm(send_elem[0].T), in_hbm(old_states))
    states = lax.all_to_all(outgoing, "dom", 0, 0)

    dims = (elements, faces, unknowns, interior, offsets, ranks, slots)
    by_face = (elements, faces, unknowns, interior)
    packed = pl.pallas_call(
        functools.partial(condense_kernel, devices, dims),
        out_shape=[jax.ShapeDtypeStruct((ranks * full + sides, SUB, LANES), bf16)] * offsets,
        in_specs=[vmem] + [hbm] * 9,
        out_specs=[vmem] * offsets,
        scratch_shapes=[
            pltpu.SMEM((faces, elements), jnp.int32),
            pltpu.SMEM((faces, elements), f32),
            pltpu.VMEM((neighbours, elements), jnp.int32),
            pltpu.VMEM((1, elements), jnp.int32),
            pltpu.VMEM((neighbours, elements), f32),
            pltpu.VMEM((unknowns, unknowns), f32),
            pltpu.VMEM((elements, nf, interior), bf16),
            pltpu.VMEM((elements, interior, interior), bf16),
            pltpu.VMEM(by_face, bf16),
            pltpu.VMEM((items, unknowns, interior), bf16),
            pltpu.VMEM((elements, EXTRA, interior), bf16),
            pltpu.VMEM((unknowns, unknowns + EXTRA), f32),
            pltpu.VMEM((ranks, unknowns, LANES), f32),
            pltpu.SMEM((offsets * ranks,), jnp.int32),
            pltpu.SMEM((offsets * ranks,), f32),
            pltpu.SMEM((offsets,), jnp.int32),
            pltpu.SemaphoreType.DMA((6,)),
            pltpu.SemaphoreType.DMA((3, elements)),
        ],
        cost_estimate=pl.CostEstimate(
            flops=2 * items * unknowns * unknowns * interior,
            bytes_accessed=2 * items * interior * 3 * unknowns,
            transcendentals=0,
        ),
        compiler_params=pltpu.CompilerParams(vmem_limit_bytes=50 * 2**20),
        name="condense",
    )(
        states.reshape(devices * slots, interior),
        in_hbm(face_shift.T),
        in_hbm(face_scale.T),
        in_hbm(recv_slot.T),
        in_hbm(intersection_count.reshape(1, elements)),
        in_hbm(intersection_weight.T),
        in_hbm(face_mass),
        in_hbm(face_coupling),
        in_hbm(interior_inverse),
        in_hbm(jnp.swapaxes(inner_coupling, 1, 2).reshape(by_face)),
    )

    order = sorted(range(offsets), key=lambda t: (t > reach, -abs(t - reach)))
    pieces = list(packed)
    for t in order:
        if t != reach:
            pieces[t] = passed_along(packed[t], "dom", t - reach)

    schur, rhs = pl.pallas_call(
        functools.partial(assemble_kernel, (owned, unknowns, offsets, ranks)),
        out_shape=[
            jax.ShapeDtypeStruct((owned, unknowns * unknowns), f32),
            jax.ShapeDtypeStruct((owned, unknowns), f32),
        ],
        in_specs=[hbm] + [vmem] * offsets,
        out_specs=[vmem, vmem],
        scratch_shapes=[
            pltpu.SMEM((offsets, 1, ranks), jnp.int32),
            pltpu.VMEM((owned + 1, SUB, width), f32),
            pltpu.SemaphoreType.DMA((1,)),
        ],
        compiler_params=pltpu.CompilerParams(vmem_limit_bytes=16 * 2**20),
        name="assemble",
    )(in_hbm(jnp.swapaxes(owner_row, 0, 1)), *pieces)
    return schur, rhs


def solution(mesh):
    in_specs = (
        P(("dom", "sub"), None),
        P(("dom", "sub"), None, None),
        P(("dom", "sub"), None),
        P(("dom", "sub")),
        P(("dom", "sub"), None),
        P(("dom", "sub"), None, None),
        P(("dom", "sub"), None, None),
        P(("dom", "sub"), None, None),
        P(),
        P(("dom", "sub"), None),
        P(("dom", "sub"), None),
        P(("dom", "sub"), None, None),
    )
    out_specs = (P(("dom", "sub"), None), P(("dom", "sub"), None))
    return jax.shard_map(
        per_device, mesh=mesh, in_specs=in_specs, out_specs=out_specs, check_vma=False
    )
```

```python
import functools

import jax
import jax.numpy as jnp
from jax import lax
from jax.experimental import pallas as pl
from jax.experimental.pallas import tpu as pltpu
from jax.sharding import PartitionSpec as P

HIGH = lax.Precision.HIGHEST
LANES = 128
SUB = 8
VMEM_BYTES = 67_043_328
AHEAD = 2
GROUP = 4
INNER_LAG = 0
EARLY = 4
EXTRA = 16
NN = (((1,), (0,)), ((), ()))
NT = (((1,), (1,)), ((), ()))
TN = (((0,), (0,)), ((), ()))


def passed_along(block, axis, distance):
    size = lax.axis_size(axis)
    route = [((i - distance) % size, i) for i in range(size)]
    return lax.ppermute(block, axis, route)


def pack_states_kernel(devices, send_hbm, old_hbm, out_ref, send, old, src, buf, sems):
    slots, offsets = send.shape
    reach = (offsets - 1) // 2
    loads = fetch((send_hbm, send), (old_hbm, old), sems=sems)
    me = lax.axis_index("dom")
    buf[...] = jnp.zeros_like(buf)
    for load in loads:
        load.wait()
    src[...] = old[...].astype(jnp.float32)
    for t in range(offsets):
        target = lax.rem(me + (t - reach + devices), devices)
        for c in range(slots):
            element = jnp.maximum(send[c, t], 0)
            buf[target, pl.ds(c, 1), :] = src[pl.ds(element, 1), :]
    out_ref[...] = buf[...].astype(jnp.bfloat16)


def tile_plan(unknowns, ranks):
    full, rest = divmod(unknowns // SUB * unknowns, LANES)
    share = LANES // rest
    return full, rest, share, -(-ranks // share)


def rest_start(unknowns, ranks):
    _, rest, share, sides = tile_plan(unknowns, ranks)
    start = rest * (ranks - share * (sides - 1))
    assert start + unknowns // SUB * ranks <= LANES
    return start


def in_hbm(array):
    return pltpu.with_memory_space_constraint(array, pltpu.HBM)


def fetch(*pairs, sems):
    loads = [
        pltpu.make_async_copy(source, target, sems.at[i])
        for i, (source, target) in enumerate(pairs)
    ]
    for load in loads:
        load.start()
    return loads


def condense_kernel(
    devices,
    dims,
    states_ref,
    shift_hbm,
    scale_hbm,
    recv_hbm,
    count_hbm,
    weight_hbm,
    mass_hbm,
    face_hbm,
    inverse_hbm,
    inner_hbm,
    *refs,
):
    elements, faces, unknowns, interior, offsets, ranks, slots = dims
    outs = refs[:offsets]
    (shift_ref, scale_ref, recv, count, weight, mass_in, rows, inverse, inner, product, tail, mass,
     square, slot_item, slot_scale, used, small_sem, sems) = refs[offsets:]
    reach = (offsets - 1) // 2
    chunk = unknowns // SUB
    full, rest, share, sides = tile_plan(unknowns, ranks)

    half = GROUP // 2
    sizes = [half] + [GROUP] * (elements // GROUP - 1) + [half]
    firsts = [sum(sizes[:i]) for i in range(len(sizes))]
    groups = len(sizes)
    chunks = elements // GROUP

    def loads(group):
        span = pl.ds(firsts[group], sizes[group])
        return (
            pltpu.make_async_copy(inverse_hbm.at[span], inverse.at[span], sems.at[0, group]),
            pltpu.make_async_copy(face_hbm.at[span], rows.at[span], sems.at[1, group]),
        )

    def inner_load(index):
        span = pl.ds(index * GROUP, GROUP)
        return pltpu.make_async_copy(inner_hbm.at[span], inner.at[span], sems.at[2, index])

    def start(group):
        for load in loads(group):
            load.start()

    small = fetch(
        (shift_hbm, shift_ref), (scale_hbm, scale_ref), (recv_hbm, recv), (count_hbm, count),
        (weight_hbm, weight), (mass_hbm, mass_in), sems=small_sem,
    )
    for group in range(AHEAD):
        start(group)
    for t in range(offsets):
        used[t] = 0
    for s in range(offsets * ranks):
        slot_item[s] = 0
        slot_scale[s] = 1.0
    mass[...] = jnp.zeros_like(mass)
    for load in small:
        load.wait()
    mass[:, :unknowns] = mass_in[...]

    me = lax.axis_index("dom")
    slot = recv[...]
    live = lax.broadcasted_iota(jnp.int32, slot.shape, 0) < count[...]
    weights = jnp.where(live, weight[...], 0.0)
    weights = weights / jnp.sum(weights, axis=0, keepdims=True)
    slot = jnp.maximum(slot, 0)
    source = lax.rem(me - slot // slots + (reach + devices), devices)
    place = source * slots + slot % slots
    total = states_ref.shape[0]
    row = lax.broadcasted_iota(jnp.int32, (total, elements), 0)
    mix = jnp.zeros((total, elements), jnp.float32)
    for k in range(slot.shape[0]):
        mix = mix + jnp.where(row == place[k : k + 1, :], weights[k : k + 1, :], 0.0)
    projected = lax.dot_general(
        mix, states_ref[...].astype(jnp.float32), TN, precision=HIGH,
        preferred_element_type=jnp.float32,
    ).astype(jnp.bfloat16)
    for e in range(elements):
        tail[e] = jnp.broadcast_to(projected[e : e + 1, :], tail.shape[1:])

    for group in range(groups):
        for load in loads(group):
            load.wait()
        if group + AHEAD < groups:
            start(group + AHEAD)
        for index in range(chunks):
            if min(index + INNER_LAG, groups - 1) == group:
                inner_load(index).start()
        for e in range(firsts[group], firsts[group] + sizes[group]):
            block = lax.dot_general(
                rows[e], inverse[e], NN, preferred_element_type=jnp.float32
            ).astype(jnp.bfloat16)
            for j in range(faces):
                item = e * faces + j
                product[item] = block[j * unknowns : (j + 1) * unknowns, :]
                shift = shift_ref[j, e] + reach
                rank = used[shift]
                used[shift] = rank + 1
                slot_item[shift * ranks + rank] = item
                slot_scale[shift * ranks + rank] = scale_ref[j, e]
    for index in range(chunks):
        inner_load(index).wait()

    lane = lax.broadcasted_iota(jnp.int32, (SUB, LANES), 1)
    turn = rest_start(unknowns, ranks) - unknowns
    for t in range(offsets):
        ends = [jnp.zeros((SUB, LANES), jnp.float32)] * sides
        for k in range(ranks):
            s = t * ranks + k
            item = slot_item[s]
            element = item // faces
            correction = lax.dot_general(
                product[item],
                jnp.concatenate([inner[element, item % faces], tail[element]], axis=0),
                NT,
                preferred_element_type=jnp.float32,
            )
            spot = s % square.shape[0]
            square[spot, :, pl.ds(0, mass.shape[1])] = slot_scale[s] * mass[...] - correction
            parts = [square[spot, pl.ds(g, SUB, stride=chunk), :] for g in range(chunk)]
            turned = [turn_lanes(p, g * unknowns) for g, p in enumerate(parts)]
            for i in range(full):
                low = i * LANES
                first = low // unknowns
                value = turned[first]
                for g in range(first + 1, min(chunk, -(-(low + LANES) // unknowns))):
                    value = jnp.where(lane >= g * unknowns - low, turned[g], value)
                outs[t][k * full + i] = value.astype(jnp.bfloat16)
            low = rest * (k % share)
            value = turn_lanes(parts[-1], (chunk - 1) * unknowns - full * LANES + low)
            inside = (lane >= low) & (lane < low + rest)
            ends[k // share] = jnp.where(inside, value, ends[k // share])
            value = jnp.zeros_like(value)
            for g in range(chunk):
                value = jnp.where(lane == unknowns + g, parts[g], value)
            ends[-1] = ends[-1] + turn_lanes(value, turn + chunk * k)
        for i in range(sides):
            outs[t][ranks * full + i] = ends[i].astype(jnp.bfloat16)


def turn_lanes(value, amount):
    amount = amount % LANES
    return pltpu.roll(value, amount, 1) if amount else value


def add_pieces(owned, unknowns, owner, offset_list, pieces, total):
    ranks = owner.shape[2]
    chunk = unknowns // SUB
    full, rest, share, sides = tile_plan(unknowns, ranks)
    lane = lax.broadcasted_iota(jnp.int32, (SUB, LANES), 1)
    last = pl.ds(full * LANES, LANES)
    for t, piece in zip(offset_list, pieces):
        ends = [piece[ranks * full + i].astype(jnp.float32) for i in range(sides)]
        for k in range(ranks):
            row = owner[t, 0, k]
            row = jnp.where(row < 0, owned, row)
            for i in range(full):
                tile = pl.ds(i * LANES, LANES)
                total[row, :, tile] = total[row, :, tile] + piece[k * full + i].astype(jnp.float32)
            tail = turn_lanes(ends[-1], unknowns - rest_start(unknowns, ranks) - chunk * k)
            tail = jnp.where(lane < rest, turn_lanes(ends[k // share], -rest * (k % share)), tail)
            total[row, :, last] = total[row, :, last] + tail


def early_kernel(owned, unknowns, offset_list, owner_in, *refs):
    pieces = refs[: len(offset_list)]
    total, owner, sems = refs[len(offset_list) :]
    loads = fetch((owner_in, owner), sems=sems)
    total[...] = jnp.zeros_like(total)
    loads[0].wait()
    add_pieces(owned, unknowns, owner, offset_list, pieces, total)


def assemble_kernel(owned, unknowns, offset_list, owner_in, early, *refs):
    pieces = refs[: len(offset_list)]
    schur_hbm, rhs_hbm, owner, total, schur, rhs, sems = refs[len(offset_list) :]
    chunk = unknowns // SUB
    width = chunk * unknowns
    last = total.shape[2] - LANES
    loads = fetch((owner_in, owner), sems=sems)
    total[...] = early[...]
    loads[0].wait()
    add_pieces(owned, unknowns, owner, offset_list, pieces, total)
    stores = []
    for group in range(owned // SUB):
        faces = pl.ds(group * SUB, SUB)
        for a in range(SUB):
            value = total[faces, a, :]
            schur[faces, a * width : (a + 1) * width] = value[:, :width]
            rhs[faces, a * chunk : (a + 1) * chunk] = value[
                :, last + unknowns : last + unknowns + chunk
            ]
        stores.append(
            pltpu.make_async_copy(schur.at[faces], schur_hbm.at[faces], sems.at[1 + group])
        )
        stores[-1].start()
    stores.append(pltpu.make_async_copy(rhs, rhs_hbm, sems.at[1 + owned // SUB]))
    stores[-1].start()
    for store in stores:
        store.wait()


def per_device(
    old_states,
    send_elem,
    recv_slot,
    intersection_count,
    intersection_weight,
    interior_inverse,
    inner_coupling,
    face_coupling,
    face_mass,
    face_scale,
    face_shift,
    owner_row,
):
    devices = lax.axis_size("dom")
    offsets, slots = send_elem.shape[1:]
    reach = (offsets - 1) // 2
    ranks = owner_row.shape[2]
    elements, interior = old_states.shape
    neighbours = recv_slot.shape[1]
    faces = face_scale.shape[1]
    unknowns = face_mass.shape[0]
    nf = faces * unknowns
    items = elements * faces
    owned = items // 2
    full, rest, share, sides = tile_plan(unknowns, ranks)
    width = (full + 1) * LANES
    vmem = pl.BlockSpec(memory_space=pltpu.VMEM)
    hbm = pl.BlockSpec(memory_space=pltpu.HBM)
    bf16, f32 = jnp.bfloat16, jnp.float32

    outgoing = pl.pallas_call(
        functools.partial(pack_states_kernel, devices),
        out_shape=jax.ShapeDtypeStruct((devices, slots, interior), bf16),
        in_specs=[hbm, hbm],
        out_specs=vmem,
        scratch_shapes=[
            pltpu.SMEM((slots, offsets), jnp.int32),
            pltpu.VMEM((elements, interior), bf16),
            pltpu.VMEM((elements, interior), f32),
            pltpu.VMEM((devices, slots, interior), f32),
            pltpu.SemaphoreType.DMA((2,)),
        ],
        compiler_params=pltpu.CompilerParams(vmem_limit_bytes=16 * 2**20),
        name="pack_states",
    )(in_hbm(send_elem[0].T), in_hbm(old_states))
    states = lax.all_to_all(outgoing, "dom", 0, 0)

    dims = (elements, faces, unknowns, interior, offsets, ranks, slots)
    by_face = (elements, faces, unknowns, interior)
    packed = pl.pallas_call(
        functools.partial(condense_kernel, devices, dims),
        out_shape=[jax.ShapeDtypeStruct((ranks * full + sides, SUB, LANES), bf16)] * offsets,
        in_specs=[vmem] + [hbm] * 9,
        out_specs=[vmem] * offsets,
        scratch_shapes=[
            pltpu.SMEM((faces, elements), jnp.int32),
            pltpu.SMEM((faces, elements), f32),
            pltpu.VMEM((neighbours, elements), jnp.int32),
            pltpu.VMEM((1, elements), jnp.int32),
            pltpu.VMEM((neighbours, elements), f32),
            pltpu.VMEM((unknowns, unknowns), f32),
            pltpu.VMEM((elements, nf, interior), bf16),
            pltpu.VMEM((elements, interior, interior), bf16),
            pltpu.VMEM(by_face, bf16),
            pltpu.VMEM((items, unknowns, interior), bf16),
            pltpu.VMEM((elements, EXTRA, interior), bf16),
            pltpu.VMEM((unknowns, unknowns + EXTRA), f32),
            pltpu.VMEM((ranks, unknowns, LANES), f32),
            pltpu.SMEM((offsets * ranks,), jnp.int32),
            pltpu.SMEM((offsets * ranks,), f32),
            pltpu.SMEM((offsets,), jnp.int32),
            pltpu.SemaphoreType.DMA((6,)),
            pltpu.SemaphoreType.DMA((3, elements)),
        ],
        cost_estimate=pl.CostEstimate(
            flops=2 * items * unknowns * unknowns * interior,
            bytes_accessed=2 * items * interior * 3 * unknowns,
            transcendentals=0,
        ),
        compiler_params=pltpu.CompilerParams(vmem_limit_bytes=50 * 2**20),
        name="condense",
    )(
        states.reshape(devices * slots, interior),
        in_hbm(face_shift.T),
        in_hbm(face_scale.T),
        in_hbm(recv_slot.T),
        in_hbm(intersection_count.reshape(1, elements)),
        in_hbm(intersection_weight.T),
        in_hbm(face_mass),
        in_hbm(face_coupling),
        in_hbm(interior_inverse),
        in_hbm(jnp.swapaxes(inner_coupling, 1, 2).reshape(by_face)),
    )

    order = sorted(range(offsets), key=lambda t: (t > reach, -abs(t - reach)))
    pieces = list(packed)
    for t in order:
        if t != reach:
            pieces[t] = passed_along(packed[t], "dom", t - reach)

    owner = jnp.swapaxes(owner_row, 0, 1)
    first = list(range(EARLY)) + [reach]
    late = [t for t in range(offsets) if t not in first]
    sums = (owned + 1, SUB, width)
    early = pl.pallas_call(
        functools.partial(early_kernel, owned, unknowns, first),
        out_shape=jax.ShapeDtypeStruct(sums, f32),
        in_specs=[vmem] + [vmem] * len(first),
        out_specs=vmem,
        scratch_shapes=[
            pltpu.SMEM((offsets, 1, ranks), jnp.int32),
            pltpu.SemaphoreType.DMA((1,)),
        ],
        compiler_params=pltpu.CompilerParams(vmem_limit_bytes=16 * 2**20),
        name="early",
    )(owner, *[pieces[t] for t in first])
    schur, rhs = pl.pallas_call(
        functools.partial(assemble_kernel, owned, unknowns, late),
        out_shape=[
            jax.ShapeDtypeStruct((owned, unknowns * unknowns), f32),
            jax.ShapeDtypeStruct((owned, unknowns), f32),
        ],
        in_specs=[vmem, vmem] + [vmem] * len(late),
        out_specs=[hbm, hbm],
        scratch_shapes=[
            pltpu.SMEM((offsets, 1, ranks), jnp.int32),
            pltpu.VMEM(sums, f32),
            pltpu.VMEM((owned, unknowns * unknowns), f32),
            pltpu.VMEM((owned, unknowns), f32),
            pltpu.SemaphoreType.DMA((2 + owned // SUB,)),
        ],
        compiler_params=pltpu.CompilerParams(vmem_limit_bytes=16 * 2**20),
        name="assemble",
    )(owner, early, *[pieces[t] for t in late])
    return schur, rhs


def solution(mesh):
    in_specs = (
        P(("dom", "sub"), None),
        P(("dom", "sub"), None, None),
        P(("dom", "sub"), None),
        P(("dom", "sub")),
        P(("dom", "sub"), None),
        P(("dom", "sub"), None, None),
        P(("dom", "sub"), None, None),
        P(("dom", "sub"), None, None),
        P(),
        P(("dom", "sub"), None),
        P(("dom", "sub"), None),
        P(("dom", "sub"), None, None),
    )
    out_specs = (P(("dom", "sub"), None), P(("dom", "sub"), None))
    return jax.shard_map(
        per_device, mesh=mesh, in_specs=in_specs, out_specs=out_specs, check_vma=False
    )
```

```python
import functools

import jax
import jax.numpy as jnp
from jax import lax
from jax.experimental import pallas as pl
from jax.experimental.pallas import tpu as pltpu
from jax.sharding import PartitionSpec as P


HIGH = lax.Precision.HIGHEST
LANES = 128
SUB = 8
AHEAD = 2
GROUP = 4

EARLY = 4
LEAD = 8
EXTRA = 16
NN = (((1,), (0,)), ((), ()))
NT = (((1,), (1,)), ((), ()))
TN = (((0,), (0,)), ((), ()))


def passed_along(block, axis, distance):
    size = lax.axis_size(axis)
    route = [((i - distance) % size, i) for i in range(size)]
    return lax.ppermute(block, axis, route)


def pack_states_kernel(devices, send_hbm, old_hbm, out_ref, send, old, src, buf, sems):
    slots, offsets = send.shape
    reach = (offsets - 1) // 2
    loads = fetch((send_hbm, send), (old_hbm, old), sems=sems)
    me = lax.axis_index("dom")
    buf[...] = jnp.zeros_like(buf)
    for load in loads:
        load.wait()
    src[...] = old[...].astype(jnp.float32)
    for t in range(offsets):
        target = lax.rem(me + (t - reach + devices), devices)
        for c in range(slots):
            element = jnp.maximum(send[c, t], 0)
            buf[target, pl.ds(c, 1), :] = src[pl.ds(element, 1), :]
    out_ref[...] = buf[...].astype(jnp.bfloat16)


def tile_plan(unknowns, ranks):
    full, rest = divmod(unknowns // SUB * unknowns, LANES)
    share = LANES // rest
    return full, rest, share, -(-ranks // share)


def rest_start(unknowns, ranks):
    _, rest, share, sides = tile_plan(unknowns, ranks)
    start = rest * (ranks - share * (sides - 1))
    assert start + unknowns // SUB * ranks <= LANES
    return start


def in_hbm(array):
    return pltpu.with_memory_space_constraint(array, pltpu.HBM)


def fetch(*pairs, sems):
    loads = [
        pltpu.make_async_copy(source, target, sems.at[i])
        for i, (source, target) in enumerate(pairs)
    ]
    for load in loads:
        load.start()
    return loads


def lead_kernel(face_hbm, inverse_hbm, out_ref, rows, inverse, sems):
    count, nf, _ = rows.shape
    unknowns = out_ref.shape[1]
    faces = nf // unknowns
    step = GROUP // 2

    def loads(first):
        span = pl.ds(first, step)
        return (
            pltpu.make_async_copy(inverse_hbm.at[span], inverse.at[span], sems.at[0, first]),
            pltpu.make_async_copy(face_hbm.at[span], rows.at[span], sems.at[1, first]),
        )

    for first in range(0, count, step):
        for load in loads(first):
            load.start()
    for first in range(0, count, step):
        for load in loads(first):
            load.wait()
        for e in range(first, first + step):
            block = lax.dot_general(
                rows[e], inverse[e], NN, preferred_element_type=jnp.float32
            ).astype(jnp.bfloat16)
            for j in range(faces):
                out_ref[e * faces + j] = block[j * unknowns : (j + 1) * unknowns, :]


def condense_kernel(
    devices,
    dims,
    states_ref,
    lead_ref,
    shift_hbm,
    scale_hbm,
    recv_hbm,
    count_hbm,
    weight_hbm,
    mass_hbm,
    face_hbm,
    inverse_hbm,
    inner_hbm,
    *refs,
):
    elements, faces, unknowns, _, offsets, ranks, slots = dims
    outs = refs[:offsets]
    (shift_ref, scale_ref, recv, count, weight, mass_in, rows, inverse, inner, product, tail, mass,
     square, slot_item, slot_scale, used, small_sem, sems) = refs[offsets:]
    reach = (offsets - 1) // 2
    chunk = unknowns // SUB
    full, rest, share, sides = tile_plan(unknowns, ranks)

    half = GROUP // 2
    lead = lead_ref.shape[0] // faces
    sizes = [half] + [GROUP] * ((elements - lead - half) // GROUP)
    sizes = sizes + [elements - lead - sum(sizes)] * (elements - lead > sum(sizes))
    firsts = [lead + sum(sizes[:i]) for i in range(len(sizes))]
    groups = len(sizes)
    chunks = elements // GROUP

    def loads(group):
        span = pl.ds(firsts[group], sizes[group])
        return (
            pltpu.make_async_copy(inverse_hbm.at[span], inverse.at[span], sems.at[0, group]),
            pltpu.make_async_copy(face_hbm.at[span], rows.at[span], sems.at[1, group]),
        )

    def inner_load(index):
        span = pl.ds(index * GROUP, GROUP)
        return pltpu.make_async_copy(inner_hbm.at[span], inner.at[span], sems.at[2, index])

    def start(group):
        for load in loads(group):
            load.start()

    small = fetch(
        (shift_hbm, shift_ref), (scale_hbm, scale_ref), (recv_hbm, recv), (count_hbm, count),
        (weight_hbm, weight), (mass_hbm, mass_in), sems=small_sem,
    )
    for group in range(AHEAD):
        start(group)
    for t in range(offsets):
        used[t] = 0
    for s in range(offsets * ranks):
        slot_item[s] = 0
        slot_scale[s] = 1.0
    mass[...] = jnp.zeros_like(mass)
    for load in small:
        load.wait()
    mass[:, :unknowns] = mass_in[...]

    me = lax.axis_index("dom")
    slot = recv[...]
    live = lax.broadcasted_iota(jnp.int32, slot.shape, 0) < count[...]
    weights = jnp.where(live, weight[...], 0.0)
    weights = weights / jnp.sum(weights, axis=0, keepdims=True)
    slot = jnp.maximum(slot, 0)
    source = lax.rem(me - slot // slots + (reach + devices), devices)
    place = source * slots + slot % slots
    total = states_ref.shape[0]
    row = lax.broadcasted_iota(jnp.int32, (total, elements), 0)
    mix = jnp.zeros((total, elements), jnp.float32)
    for k in range(slot.shape[0]):
        mix = mix + jnp.where(row == place[k : k + 1, :], weights[k : k + 1, :], 0.0)
    projected = lax.dot_general(
        mix, states_ref[...].astype(jnp.float32), TN, precision=HIGH,
        preferred_element_type=jnp.float32,
    ).astype(jnp.bfloat16)
    for e in range(elements):
        tail[e] = jnp.broadcast_to(projected[e : e + 1, :], tail.shape[1:])

    def assign(e):
        for j in range(faces):
            shift = shift_ref[j, e] + reach
            rank = used[shift]
            used[shift] = rank + 1
            slot_item[shift * ranks + rank] = e * faces + j
            slot_scale[shift * ranks + rank] = scale_ref[j, e]

    product[pl.ds(0, lead * faces)] = lead_ref[...]
    for group in range(groups):
        for load in loads(group):
            load.wait()
        if group == 0:
            for e in range(lead):
                assign(e)
        if group + AHEAD < groups:
            start(group + AHEAD)
        for index in range(chunks):
            if index * (groups - 1) // chunks == group:
                inner_load(index).start()
        for e in range(firsts[group], firsts[group] + sizes[group]):
            block = lax.dot_general(
                rows[e], inverse[e], NN, preferred_element_type=jnp.float32
            ).astype(jnp.bfloat16)
            for j in range(faces):
                item = e * faces + j
                product[item] = block[j * unknowns : (j + 1) * unknowns, :]
            assign(e)
    for index in range(chunks):
        inner_load(index).wait()

    lane = lax.broadcasted_iota(jnp.int32, (SUB, LANES), 1)
    turn = rest_start(unknowns, ranks) - unknowns
    for t in range(offsets):
        ends = [jnp.zeros((SUB, LANES), jnp.float32)] * sides
        for k in range(ranks):
            s = t * ranks + k
            item = slot_item[s]
            element = item // faces
            correction = lax.dot_general(
                product[item],
                jnp.concatenate([inner[element, item % faces], tail[element]], axis=0),
                NT,
                preferred_element_type=jnp.float32,
            )
            spot = s % square.shape[0]
            square[spot, :, pl.ds(0, mass.shape[1])] = slot_scale[s] * mass[...] - correction
            parts = [square[spot, pl.ds(g, SUB, stride=chunk), :] for g in range(chunk)]
            turned = [turn_lanes(p, g * unknowns) for g, p in enumerate(parts)]
            for i in range(full):
                low = i * LANES
                first = low // unknowns
                value = turned[first]
                for g in range(first + 1, min(chunk, -(-(low + LANES) // unknowns))):
                    value = jnp.where(lane >= g * unknowns - low, turned[g], value)
                outs[t][k * full + i] = value.astype(jnp.bfloat16)
            low = rest * (k % share)
            value = turn_lanes(parts[-1], (chunk - 1) * unknowns - full * LANES + low)
            inside = (lane >= low) & (lane < low + rest)
            ends[k // share] = jnp.where(inside, value, ends[k // share])
            value = jnp.zeros_like(value)
            for g in range(chunk):
                value = jnp.where(lane == unknowns + g, parts[g], value)
            ends[-1] = ends[-1] + turn_lanes(value, turn + chunk * k)
        for i in range(sides):
            outs[t][ranks * full + i] = ends[i].astype(jnp.bfloat16)


def turn_lanes(value, amount):
    amount = amount % LANES
    return pltpu.roll(value, amount, 1) if amount else value


def add_pieces(owned, unknowns, owner, offset_list, pieces, total):
    ranks = owner.shape[2]
    chunk = unknowns // SUB
    full, rest, share, sides = tile_plan(unknowns, ranks)
    lane = lax.broadcasted_iota(jnp.int32, (SUB, LANES), 1)
    last = pl.ds(full * LANES, LANES)
    for t, piece in zip(offset_list, pieces):
        ends = [piece[ranks * full + i].astype(jnp.float32) for i in range(sides)]
        for k in range(ranks):
            row = owner[t, 0, k]
            row = jnp.where(row < 0, owned, row)
            for i in range(full):
                tile = pl.ds(i * LANES, LANES)
                total[row, :, tile] = total[row, :, tile] + piece[k * full + i].astype(jnp.float32)
            tail = turn_lanes(ends[-1], unknowns - rest_start(unknowns, ranks) - chunk * k)
            tail = jnp.where(lane < rest, turn_lanes(ends[k // share], -rest * (k % share)), tail)
            total[row, :, last] = total[row, :, last] + tail


def early_kernel(owned, unknowns, offset_list, owner_in, *refs):
    pieces = refs[: len(offset_list)]
    total, owner, sems = refs[len(offset_list) :]
    loads = fetch((owner_in, owner), sems=sems)
    total[...] = jnp.zeros_like(total)
    loads[0].wait()
    add_pieces(owned, unknowns, owner, offset_list, pieces, total)


def assemble_kernel(owned, unknowns, offset_list, owner_in, early, *refs):
    pieces = refs[: len(offset_list)]
    schur_hbm, rhs_hbm, owner, total, schur, rhs, sems = refs[len(offset_list) :]
    chunk = unknowns // SUB
    width = chunk * unknowns
    last = total.shape[2] - LANES
    loads = fetch((owner_in, owner), sems=sems)
    total[...] = early[...]
    loads[0].wait()
    add_pieces(owned, unknowns, owner, offset_list, pieces, total)
    stores = []
    for group in range(owned // SUB):
        faces = pl.ds(group * SUB, SUB)
        for a in range(SUB):
            value = total[faces, a, :]
            schur[faces, a * width : (a + 1) * width] = value[:, :width]
            rhs[faces, a * chunk : (a + 1) * chunk] = value[
                :, last + unknowns : last + unknowns + chunk
            ]
        stores.append(
            pltpu.make_async_copy(schur.at[faces], schur_hbm.at[faces], sems.at[1 + group])
        )
        stores[-1].start()
    stores.append(pltpu.make_async_copy(rhs, rhs_hbm, sems.at[1 + owned // SUB]))
    stores[-1].start()
    for store in stores:
        store.wait()


def per_device(
    old_states,
    send_elem,
    recv_slot,
    intersection_count,
    intersection_weight,
    interior_inverse,
    inner_coupling,
    face_coupling,
    face_mass,
    face_scale,
    face_shift,
    owner_row,
):
    devices = lax.axis_size("dom")
    offsets, slots = send_elem.shape[1:]
    reach = (offsets - 1) // 2
    ranks = owner_row.shape[2]
    elements, interior = old_states.shape
    neighbours = recv_slot.shape[1]
    faces = face_scale.shape[1]
    unknowns = face_mass.shape[0]
    nf = faces * unknowns
    items = elements * faces
    owned = items // 2
    full, _, _, sides = tile_plan(unknowns, ranks)
    width = (full + 1) * LANES
    vmem = pl.BlockSpec(memory_space=pltpu.VMEM)
    hbm = pl.BlockSpec(memory_space=pltpu.HBM)
    bf16, f32 = jnp.bfloat16, jnp.float32

    outgoing = pl.pallas_call(
        functools.partial(pack_states_kernel, devices),
        out_shape=jax.ShapeDtypeStruct((devices, slots, interior), bf16),
        in_specs=[hbm, hbm],
        out_specs=vmem,
        scratch_shapes=[
            pltpu.SMEM((slots, offsets), jnp.int32),
            pltpu.VMEM((elements, interior), bf16),
            pltpu.VMEM((elements, interior), f32),
            pltpu.VMEM((devices, slots, interior), f32),
            pltpu.SemaphoreType.DMA((2,)),
        ],
        compiler_params=pltpu.CompilerParams(vmem_limit_bytes=16 * 2**20),
        name="pack_states",
    )(in_hbm(send_elem[0].T), in_hbm(old_states))
    states = lax.all_to_all(outgoing, "dom", 0, 0)

    dims = (elements, faces, unknowns, interior, offsets, ranks, slots)
    by_face = (elements, faces, unknowns, interior)
    count = min(LEAD, elements - GROUP)
    lead = pl.pallas_call(
        lead_kernel,
        out_shape=jax.ShapeDtypeStruct((count * faces, unknowns, interior), bf16),
        in_specs=[hbm] * 2,
        out_specs=vmem,
        scratch_shapes=[
            pltpu.VMEM((count, nf, interior), bf16),
            pltpu.VMEM((count, interior, interior), bf16),
            pltpu.SemaphoreType.DMA((2, count)),
        ],
        cost_estimate=pl.CostEstimate(
            flops=2 * count * nf * interior * interior,
            bytes_accessed=2 * count * interior * (interior + 2 * nf),
            transcendentals=0,
        ),
        compiler_params=pltpu.CompilerParams(vmem_limit_bytes=24 * 2**20),
        name="lead",
    )(in_hbm(face_coupling), in_hbm(interior_inverse))
    packed = pl.pallas_call(
        functools.partial(condense_kernel, devices, dims),
        out_shape=[jax.ShapeDtypeStruct((ranks * full + sides, SUB, LANES), bf16)] * offsets,
        in_specs=[vmem] * 2 + [hbm] * 9,
        out_specs=[vmem] * offsets,
        scratch_shapes=[
            pltpu.SMEM((faces, elements), jnp.int32),
            pltpu.SMEM((faces, elements), f32),
            pltpu.VMEM((neighbours, elements), jnp.int32),
            pltpu.VMEM((1, elements), jnp.int32),
            pltpu.VMEM((neighbours, elements), f32),
            pltpu.VMEM((unknowns, unknowns), f32),
            pltpu.VMEM((elements, nf, interior), bf16),
            pltpu.VMEM((elements, interior, interior), bf16),
            pltpu.VMEM(by_face, bf16),
            pltpu.VMEM((items, unknowns, interior), bf16),
            pltpu.VMEM((elements, EXTRA, interior), bf16),
            pltpu.VMEM((unknowns, unknowns + EXTRA), f32),
            pltpu.VMEM((ranks, unknowns, LANES), f32),
            pltpu.SMEM((offsets * ranks,), jnp.int32),
            pltpu.SMEM((offsets * ranks,), f32),
            pltpu.SMEM((offsets,), jnp.int32),
            pltpu.SemaphoreType.DMA((6,)),
            pltpu.SemaphoreType.DMA((3, elements)),
        ],
        cost_estimate=pl.CostEstimate(
            flops=2 * items * unknowns * unknowns * interior,
            bytes_accessed=2 * items * interior * 3 * unknowns,
            transcendentals=0,
        ),
        compiler_params=pltpu.CompilerParams(vmem_limit_bytes=50 * 2**20),
        name="condense",
    )(
        states.reshape(devices * slots, interior),
        lead,
        in_hbm(face_shift.T),
        in_hbm(face_scale.T),
        in_hbm(recv_slot.T),
        in_hbm(intersection_count.reshape(1, elements)),
        in_hbm(intersection_weight.T),
        in_hbm(face_mass),
        in_hbm(face_coupling),
        in_hbm(interior_inverse),
        in_hbm(jnp.swapaxes(inner_coupling, 1, 2).reshape(by_face)),
    )

    pieces = list(packed)
    for t in range(offsets):
        if t != reach:
            pieces[t] = passed_along(packed[t], "dom", t - reach)

    owner = jnp.swapaxes(owner_row, 0, 1)
    first = list(range(EARLY)) + [reach]
    late = [t for t in range(offsets) if t not in first]
    sums = (owned + 1, SUB, width)
    early = pl.pallas_call(
        functools.partial(early_kernel, owned, unknowns, first),
        out_shape=jax.ShapeDtypeStruct(sums, f32),
        in_specs=[vmem] + [vmem] * len(first),
        out_specs=vmem,
        scratch_shapes=[
            pltpu.SMEM((offsets, 1, ranks), jnp.int32),
            pltpu.SemaphoreType.DMA((1,)),
        ],
        compiler_params=pltpu.CompilerParams(vmem_limit_bytes=16 * 2**20),
        name="early",
    )(owner, *[pieces[t] for t in first])
    schur, rhs = pl.pallas_call(
        functools.partial(assemble_kernel, owned, unknowns, late),
        out_shape=[
            jax.ShapeDtypeStruct((owned, unknowns * unknowns), f32),
            jax.ShapeDtypeStruct((owned, unknowns), f32),
        ],
        in_specs=[vmem, vmem] + [vmem] * len(late),
        out_specs=[hbm, hbm],
        scratch_shapes=[
            pltpu.SMEM((offsets, 1, ranks), jnp.int32),
            pltpu.VMEM(sums, f32),
            pltpu.VMEM((owned, unknowns * unknowns), f32),
            pltpu.VMEM((owned, unknowns), f32),
            pltpu.SemaphoreType.DMA((2 + owned // SUB,)),
        ],
        compiler_params=pltpu.CompilerParams(vmem_limit_bytes=16 * 2**20),
        name="assemble",
    )(owner, early, *[pieces[t] for t in late])
    return schur, rhs


def solution(mesh):
    in_specs = (
        P(("dom", "sub"), None),
        P(("dom", "sub"), None, None),
        P(("dom", "sub"), None),
        P(("dom", "sub")),
        P(("dom", "sub"), None),
        P(("dom", "sub"), None, None),
        P(("dom", "sub"), None, None),
        P(("dom", "sub"), None, None),
        P(),
        P(("dom", "sub"), None),
        P(("dom", "sub"), None),
        P(("dom", "sub"), None, None),
    )
    out_specs = (P(("dom", "sub"), None), P(("dom", "sub"), None))
    return jax.shard_map(
        per_device, mesh=mesh, in_specs=in_specs, out_specs=out_specs, check_vma=False
    )
```
